32 devices in a mesh: ep: 16 (over z, y, x), tp: 2 (over core).
Axes of the slice: x: 2, y: 2, z: 4, core: 2. Of those that a mesh axis runs over, the one named last changes fastest.
Arguments:
- tokens: bfloat16 [2048, 2048], P('ep', 'tp'), may hold values from -6 to 6
- cotangent: bfloat16 [2048, 2048], P('ep', 'tp'), may hold values from -6 to 6
- expert_ids: int32 [2048, 6], P('ep'), may hold values from 0 to 15, all different within a row; in each aligned block of 128 rows (0 to 127, 128 to 255, ...) at most 64 rows name the same one
- gate_values: float32 [2048, 6], P('ep'), may hold values from 0.1 to 1
- w_gate: bfloat16 [16, 1408, 2048], P('ep', 'tp'), may hold values from -0.125 to 0.125
- w_up: bfloat16 [16, 1408, 2048], P('ep', 'tp'), may hold values from -0.125 to 0.125
- w_down: bfloat16 [16, 1408, 2048], P('ep', 'tp'), may hold values from -0.15625 to 0.15625
Outputs:
- input_grad: bfloat16 [2048, 2048], P('ep', 'tp')
- grad_gate: bfloat16 [16, 1408, 2048], P('ep', 'tp')
- grad_up: bfloat16 [16, 1408, 2048], P('ep', 'tp')
- grad_down: bfloat16 [16, 1408, 2048], P('ep', 'tp')
The draws below stay inside these ranges and needn't reach their ends.
Inputs may be any that keep to these rules, and one draw needn't show every extreme that they name: `expert_ids`: each token names 6 different experts. Among the 128 tokens of one group, no expert is named more than 64 times.
All inputs are finite; a program needn't handle non-finite values.
Results may differ from the reference program's by a relative error of at most 0.017.
Values may be sent and summed in bfloat16 or wider, within the bound.
A program may use at most 64 MiB of HBM per device.

```python
import math
from functools import partial
import jax
import jax.numpy as jnp
import numpy as np
from jax import lax

D = 2048
FF = 1408
TOP = 6
TOK_DEV = 128
EXPERTS = 16
CAP = 64
TOKENS = 2048
N_EP = 16
N_TP = 2


def block_levels(stream_key, extent, cuts, low, high):
    def one(axis_at, shards_of):
        heights = jax.random.uniform(jax.random.fold_in(jax.random.fold_in(stream_key, 6), axis_at), (shards_of,), jnp.float32, low / len(cuts), high / len(cuts))
        return jnp.repeat(jnp.exp(heights), extent[axis_at] // shards_of).reshape((-1,) + (1,) * (len(extent) - axis_at - 1))

    gain = one(*cuts[0])
    for cut in cuts[1:]:
        gain = gain * one(*cut)
    return gain


def assign_block(key, own, number, rows, amount, top, bound, skew):
    ranking = jax.random.permutation(key, amount)
    packed, usual = load_shares(amount, rows * top, bound, skew, True), load_shares(amount, rows * top, bound, skew, False)
    places = jnp.arange(amount)

    def named(lengths, turn):
        used = int((lengths > 0).sum())
        fixed = max(1, used // 4)
        moved = fixed + (places - fixed + turn * (used - fixed)) % max(1, amount - fixed)
        return jnp.zeros((amount,), jnp.int32).at[ranking[jnp.where(places < fixed, places, moved)]].set(jnp.asarray(lengths, jnp.int32))

    lengths = jnp.where(number % 4 == 0, named(packed, number // 4), named(usual, number - number // 4 - 1))
    mixed = jax.random.permutation(jax.random.fold_in(own, 3), amount)
    giver, taker = mixed[0:amount // 2 * 2:2], mixed[1:amount // 2 * 2:2]
    slack = jnp.minimum(lengths[giver] - 1, bound - lengths[taker]) // 2
    slack = jnp.where((giver == ranking[0]) | (taker == ranking[0]) | (lengths[taker] == 0), 0, jnp.maximum(slack, 0))
    moved = jax.random.randint(jax.random.fold_in(own, 4), (amount // 2,), 0, 1 << 20) % (slack + 1)
    lengths = lengths.at[giver].add(-moved).at[taker].add(moved)
    items = jnp.searchsorted(jnp.cumsum(lengths), jnp.arange(rows * top), side="right").astype(jnp.int32)
    grid = items.reshape(top, rows).T
    grid = grid[jax.random.permutation(jax.random.fold_in(own, 1), rows)]
    turn = jax.random.randint(jax.random.fold_in(own, 2), (rows, 1), 0, top)
    return jnp.take_along_axis(grid, (jnp.arange(top)[None, :] + turn) % top, axis=1)


def load_shares(count, total, reach, lean, full):
    loads = [(1 << 20) // math.isqrt(standing ** lean) + 1 for standing in range(1, count + 1)]
    largest = reach if full else min(reach, max(-(-total // count), total * loads[0] // sum(loads)))
    least = 1 if total - largest >= count - 1 else 0
    holding, spare = [largest] + [least] * (count - 1), total - largest - least * (count - 1)
    while spare > 0:
        movable = [i for i in range(1, count) if holding[i] < largest] or [i for i in range(1, count) if holding[i] < reach]
        whole, budget = sum([loads[i] for i in movable]), spare
        for i in movable:
            addition = min(reach - holding[i], max(1, budget * loads[i] // whole), spare)
            holding[i] = holding[i] + addition
            spare = spare - addition
    return np.array(holding)


def scatter_about(rng, extent, deviation, reach, pieces=(), kind=jnp.bfloat16):
    result = jax.random.normal(rng, extent, jnp.float32) * deviation
    if len(pieces) > 0:
        result = block_levels(rng, extent, pieces, -0.22, 0.18) * result
    return jnp.clip(result, min=-reach, max=reach).astype(kind)


def setup_inputs(seed: int = 0) -> dict:
    streams_of = jax.random.split(jax.random.key(seed), 8)
    tokens = scatter_about(streams_of[0], (TOKENS, D), 1.0, 6.0, ((0, 16), (1, 2)))
    cotangent = scatter_about(streams_of[1], (TOKENS, D), 1.0, 6.0, ((0, 16), (1, 2)))
    expert_ids_keys = jax.random.split(jax.random.fold_in(streams_of[2], 1), TOKENS // TOK_DEV)
    expert_ids_turns = jax.random.permutation(jax.random.fold_in(streams_of[2], 3), TOKENS // TOK_DEV)
    expert_ids = jax.vmap(lambda own, number: assign_block(jax.random.fold_in(streams_of[2], 2), own, number, TOK_DEV, EXPERTS, TOP, CAP, 2))(expert_ids_keys, expert_ids_turns).reshape((TOKENS, TOP))
    gate_values = jnp.clip(0.1 + 0.9 * jax.random.uniform(streams_of[3], (TOKENS, TOP), jnp.float32) ** block_levels(streams_of[3], (TOKENS, TOP), ((0, 16),), -0.2, 0.2), 0.1, 1.0)
    w_gate = scatter_about(streams_of[4], (EXPERTS, FF, D), D ** -0.5, 0.125, ((0, 16), (1, 2)))
    w_up = scatter_about(streams_of[5], (EXPERTS, FF, D), D ** -0.5, 0.125, ((0, 16), (1, 2)))
    w_down = scatter_about(streams_of[6], (EXPERTS, FF, D), FF ** -0.5, 0.15625, ((0, 16), (1, 2)))
    return dict(tokens=tokens, cotangent=cotangent, expert_ids=expert_ids, gate_values=gate_values, w_gate=w_gate, w_up=w_up, w_down=w_down)


def slot_numbers(flat_ids, experts):
    onehot = (flat_ids[:, None] == jnp.arange(experts, dtype=jnp.int32)[None, :]).astype(jnp.int32)
    before = jnp.cumsum(onehot, axis=0) - onehot
    return jnp.sum(before * onehot, axis=1).astype(jnp.int32)


def pair_table(expert_ids, experts, capacity):
    flat_ids = expert_ids.reshape(-1).astype(jnp.int32)
    position = (flat_ids * capacity + slot_numbers(flat_ids, experts)).astype(jnp.int32)
    matches = position[None, :] == jnp.arange(experts * capacity, dtype=jnp.int32)[:, None]
    usable = jnp.any(matches, axis=1)
    numbers = jnp.arange(flat_ids.shape[0], dtype=jnp.int32)[None, :]
    pair_index = jnp.sum(jnp.where(matches, numbers, 0), axis=1).astype(jnp.int32)
    return pair_index, usable, position


def dispatch_rows(features, cotangent, gate_values, pair_index, usable, top_count):
    token_index = (pair_index // top_count).astype(jnp.int32)
    feature_rows = jnp.where(usable[:, None], features[token_index], jnp.zeros((), features.dtype))
    scaled = gate_values.reshape(-1)[pair_index][:, None] * cotangent[token_index].astype(jnp.float32)
    cotangent_rows = jnp.where(usable[:, None], scaled, jnp.zeros((), jnp.float32)).astype(jnp.bfloat16)
    return feature_rows, cotangent_rows


def one_expert(inputs):
    expert_inputs, expert_cotangent, gate_weight, up_weight, down_weight = inputs
    row_count = expert_inputs.shape[0]
    gate_pre = jnp.dot(expert_inputs, gate_weight.T, preferred_element_type=jnp.float32)
    up_proj = jnp.dot(expert_inputs, up_weight.T, preferred_element_type=jnp.float32)
    sigmoid_gate = jax.nn.sigmoid(gate_pre)
    swish_value = gate_pre * sigmoid_gate
    hidden = (swish_value * up_proj).astype(jnp.bfloat16)
    hidden_grad = jnp.dot(expert_cotangent, down_weight.T, preferred_element_type=jnp.float32)
    gate_grad = (hidden_grad * up_proj * sigmoid_gate * (1.0 + gate_pre * (1.0 - sigmoid_gate))).astype(jnp.bfloat16)
    up_grad = (hidden_grad * swish_value).astype(jnp.bfloat16)
    grad_gate = jnp.dot(gate_grad.T, expert_inputs, preferred_element_type=jnp.float32).astype(jnp.bfloat16)
    grad_up = jnp.dot(up_grad.T, expert_inputs, preferred_element_type=jnp.float32).astype(jnp.bfloat16)
    grad_down = jnp.dot(hidden.T, expert_cotangent, preferred_element_type=jnp.float32).astype(jnp.bfloat16)
    slice_units = FF // N_TP
    gate_slices = gate_grad.astype(jnp.float32).reshape(row_count, N_TP, slice_units)
    up_slices = up_grad.astype(jnp.float32).reshape(row_count, N_TP, slice_units)
    gate_blocks = gate_weight.astype(jnp.float32).reshape(N_TP, slice_units, D)
    up_blocks = up_weight.astype(jnp.float32).reshape(N_TP, slice_units, D)
    terms = jnp.einsum("rtf,tfd->trd", gate_slices, gate_blocks, precision=lax.Precision.HIGHEST)
    terms = terms + jnp.einsum("rtf,tfd->trd", up_slices, up_blocks, precision=lax.Precision.HIGHEST)
    rounded = lax.optimization_barrier(terms.astype(jnp.bfloat16))
    input_rows = jnp.sum(rounded.astype(jnp.float32), axis=0).astype(jnp.bfloat16)
    return grad_gate, grad_up, grad_down, input_rows


def combine_rows(returned, position):
    picked = returned[position].astype(jnp.float32)
    return jnp.sum(picked.reshape(TOK_DEV, TOP, D), axis=1).astype(jnp.bfloat16)


def reference(tokens, cotangent, expert_ids, gate_values, w_gate, w_up, w_down):
    experts = N_EP
    pair_index, usable, position = jax.vmap(partial(pair_table, experts=experts, capacity=CAP))(expert_ids.reshape(N_EP, TOK_DEV, TOP))
    feature_rows, cotangent_rows = jax.vmap(partial(dispatch_rows, top_count=TOP))(
        tokens.reshape(N_EP, TOK_DEV, D), cotangent.reshape(N_EP, TOK_DEV, D),
        gate_values.reshape(N_EP, TOK_DEV, TOP), pair_index, usable)
    feature_rows = jnp.swapaxes(feature_rows.reshape(N_EP, experts, CAP, D), 0, 1).reshape(experts, N_EP * CAP, D)
    cotangent_rows = jnp.swapaxes(cotangent_rows.reshape(N_EP, experts, CAP, D), 0, 1).reshape(experts, N_EP * CAP, D)
    grad_gate, grad_up, grad_down, input_rows = lax.map(one_expert, (feature_rows, cotangent_rows, w_gate, w_up, w_down))
    returned = jnp.swapaxes(input_rows.reshape(experts, N_EP, CAP, D), 0, 1).reshape(N_EP, experts * CAP, D)
    input_grad = jax.vmap(combine_rows)(returned, position).reshape(TOKENS, D)
    return input_grad, grad_gate, grad_up, grad_down
```

```python
import functools
import jax
import jax.numpy as jnp
from jax import lax
from jax.experimental import pallas as pl
from jax.experimental.pallas import tpu as pltpu
from jax.sharding import PartitionSpec as P


def outer_factor(count):
    outer = 1
    while outer * 2 * outer * 2 <= count and count % (outer * 2) == 0:
        outer *= 2
    return outer


def nt(left, right):
    return lax.dot_general(
        left, right, (((1,), (1,)), ((), ())), preferred_element_type=jnp.float32
    )


def tn(left, right):
    return lax.dot_general(
        left, right, (((0,), (0,)), ((), ())), preferred_element_type=jnp.float32
    )


def nn(left, right):
    return jnp.dot(left, right, preferred_element_type=jnp.float32)


def kernel(
    nz, npl, ntp, cap,
    tok_hbm, cot_hbm, ids_hbm, gat_hbm, wg_hbm, wu_hbm, wd_hbm,
    ig, gg, gu, gd,
    tok, cot, ids, gat, zx, zc, zi, zg,
    oh, grow, sx, sc, xe, ge, wg, wu, wd, at, bt, ht, dat, dbt,
    red, redr, rows, rowr, part, partr,
    s_i, s_w, zs, zr, ps, pr, ls, ts, tr, ds, dr, rs, rr, rl, qs, qr,
):
    ep = lax.axis_index("ep")
    c = lax.axis_index("tp")
    z = ep // npl
    p = ep % npl
    width = tok.shape[1]
    batch = npl * cap
    half = max(1, nz // 2)
    upper = z // half if nz > 1 else 0
    w = z + upper * (nz - 1 - 2 * z)
    inner = w > 0

    def mirror(v):
        return v + upper * (nz - 1 - 2 * v)

    def source(i):
        over = (w + i) // nz
        return mirror((1 - over) * (w + i) + over * (nz - 1 - i))

    def zdev(j):
        return {"ep": ((z + j) % nz) * npl + p}

    def pdev(d):
        return {"ep": z * npl + (p + d) % npl}

    def tdev(d):
        return {"tp": (c + d) % ntp}

    def cols(core):
        return pl.ds(pl.multiple_of(core * width, width), width)

    def remote(src, dst, ssem, rsem, dev):
        return pltpu.make_async_remote_copy(
            src_ref=src, dst_ref=dst, send_sem=ssem, recv_sem=rsem,
            device_id=dev, device_id_type=pl.DeviceIdType.MESH,
        )

    inputs = [
        pltpu.make_async_copy(h, v, s_i.at[i])
        for i, (h, v) in enumerate(
            ((ids_hbm, ids), (gat_hbm, gat), (tok_hbm, tok), (cot_hbm, cot))
        )
    ]
    for copy in inputs:
        copy.start()

    barrier = pltpu.get_barrier_semaphore()
    peers = [{"ep": mirror(w + 1) * npl + p}] if nz > 1 else []
    peers += [pdev(d) for d in range(1, npl)]
    peers += [tdev(d) for d in range(1, ntp)]

    def greet(dev):
        pl.semaphore_signal(barrier, inc=1, device_id=dev, device_id_type=pl.DeviceIdType.MESH)

    for dev in peers:
        greet(dev)
    if nz > 1:

        @pl.when(inner)
        def _():
            greet({"ep": mirror(w - 1) * npl + p})

    pl.semaphore_wait(barrier, len(peers) + (w + nz - 1) // nz)

    zown = (ids, gat, tok, cot)
    zin = (zi, zg, zx, zc)

    def zsend(kind, block, to):
        slot = mirror(block)
        return remote(
            zin[kind].at[slot], zin[kind].at[slot], zs.at[kind, slot], zr.at[kind, slot],
            {"ep": mirror(to) * npl + p},
        )

    def zfirst(kind, side):
        sem = zs.at[kind, z if side > 0 else nz]
        return remote(
            zown[kind], zin[kind].at[z], sem, zr.at[kind, z], {"ep": mirror(w + side) * npl + p}
        )

    def relays(k):
        found = []
        if k < nz:
            found.append((inner if k <= nz - half else inner & (w + k < nz), k, -1))
        if k < half:
            found.append((w >= k, -k, 1))
        return found

    for kind in range(4):
        inputs[kind].wait()
        if nz > 1:
            zfirst(kind, 1).start()

            @pl.when(inner)
            def _():
                zfirst(kind, -1).start()

    weights = [
        pltpu.make_async_copy(h.at[0], v, s_w.at[i])
        for i, (h, v) in enumerate(((wg_hbm, wg), (wu_hbm, wu), (wd_hbm, wd)))
    ]
    for copy in weights:
        copy.start()

    def kinds(kind):
        return (0, 1, 2) if kind == 0 else (3,)

    def early(kind, k):
        for holds, off, side in relays(k):

            @pl.when(holds)
            def _():
                for part_ in kinds(kind):
                    copy = zsend(part_, w + off, w + side)
                    copy.wait_recv()
                    copy.start()

    def late(kind, i):
        @pl.when(w == 0)
        def _():
            for part_ in kinds(kind):
                zsend(part_, i, w).wait_recv()

    ntok = ids.shape[1]
    before = (
        lax.broadcasted_iota(jnp.int32, (ntok, ntok), 0)
        < lax.broadcasted_iota(jnp.int32, (ntok, ntok), 1)
    ).astype(jnp.bfloat16)
    slot_iota = lax.broadcasted_iota(jnp.int32, (cap, ntok), 0).astype(jnp.float32)

    def build(j):
        named = ids[...] if j == 0 else zi[source(j)]
        gates = gat[...] if j == 0 else zg[source(j)]
        for d in range(npl):
            hit = named == z * npl + (p + d) % npl
            has = jnp.sum(jnp.where(hit, 1.0, 0.0), axis=0, keepdims=True)
            gate = jnp.sum(jnp.where(hit, gates, 0.0), axis=0, keepdims=True)
            pos = nn(jnp.broadcast_to(has, (16, ntok)).astype(jnp.bfloat16), before)[0:1]
            sel = jnp.where(slot_iota == pos, 1.0, 0.0) * has
            oh[j, d * cap:(d + 1) * cap, :] = sel.astype(jnp.bfloat16)
            grow[j, d * cap:(d + 1) * cap, :] = jnp.sum(sel * gate, axis=1, keepdims=True)

    def pcopy(kind, j, d):
        src, dst = ((sx, xe), (sc, ge))[kind]
        lines = pl.ds(j * batch + d * cap, cap)
        s, t = src.at[j, pl.ds(d * cap, cap), :], dst.at[lines, cols(c)]
        if d == 0:
            return pltpu.make_async_copy(s, t, ls.at[kind, j])
        return remote(s, t, ps.at[kind, j, d], pr.at[kind, j, d], pdev(d))

    def send_x(j):
        if j:
            late(0, j)
        build(j)
        block = tok[...] if j == 0 else zx[source(j)]
        sx[j] = nn(oh[j], block).astype(jnp.bfloat16)
        for d in range(1, npl):
            pcopy(0, j, d).start()
        pcopy(0, j, 0).start()

    def send_c(j):
        if j:
            late(1, j)
        block = cot[...] if j == 0 else zc[source(j)]
        sc[j] = (nn(oh[j], block) * grow[j]).astype(jnp.bfloat16)
        for d in range(1, npl):
            pcopy(1, j, d).start()
        pcopy(1, j, 0).start()

    def tcopy(kind, j, d, q, owner):
        buf = (xe, ge)[kind]
        view = buf.at[pl.ds(j * batch + q * cap, cap), cols(owner)]
        return remote(view, view, ts.at[kind, j, q, d], tr.at[kind, j, q, d], tdev(d))

    def forward(kind, j):
        for q in range(npl):
            if q:
                pcopy(kind, j, q).wait_recv()
            else:
                pcopy(kind, j, 0).wait()
            for d in range(1, ntp):
                tcopy(kind, j, d, q, c).start()

    def arrive(kind, j):
        for q in range(npl):
            for d in range(1, ntp):
                tcopy(kind, j, d, q, (c + ntp - d) % ntp).wait_recv()

    def up(j):
        arrive(0, j)
        x = xe[j * batch:(j + 1) * batch, :]
        at[:, j * batch:(j + 1) * batch] = nt(wg[...], x)
        bt[:, j * batch:(j + 1) * batch] = nt(wu[...], x)

    def dcopy(j, d):
        return remote(
            red.at[j, :, cols((c + d) % ntp)], redr.at[j, d],
            ds.at[j, d], dr.at[j, d], tdev(d),
        )

    def down(j):
        arrive(1, j)
        lines = slice(j * batch, (j + 1) * batch)
        dh = nt(wd[...], ge[lines, :])
        a, b = at[:, lines], bt[:, lines]
        s = jax.nn.sigmoid(a)
        swish = a * s
        ht[:, lines] = (swish * b).astype(jnp.bfloat16)
        da = (dh * b * s * (1.0 + a * (1.0 - s))).astype(jnp.bfloat16)
        db = (dh * swish).astype(jnp.bfloat16)
        dat[:, lines] = da
        dbt[:, lines] = db
        for d in [*range(1, ntp), 0]:
            here = cols((c + d) % ntp)
            red[j, :, here] = (tn(da, wg[:, here]) + tn(db, wu[:, here])).astype(jnp.bfloat16)
            if d:
                dcopy(j, d).start()

    def rcopy(j, d):
        lines = pl.ds(d * cap, cap)
        s, t = rows.at[j, lines, :], rowr.at[j, lines, :]
        if d == 0:
            return pltpu.make_async_copy(s, t, rl.at[j])
        return remote(s, t, rs.at[j, d], rr.at[j, d], pdev(npl - d))

    def back(j):
        total = red[j, :, cols(c)].astype(jnp.float32)
        for d in range(1, ntp):
            dcopy(j, d).wait_recv()
            total = total + redr[j, d].astype(jnp.float32)
        rows[j] = total.astype(jnp.bfloat16)
        for d in range(1, npl):
            rcopy(j, d).start()
        rcopy(j, 0).start()

    def qcopy(j):
        return remote(
            part.at[j], partr.at[z], qs.at[j], qr.at[z], {"ep": source(j) * npl + p}
        )

    def qwait(j):
        here = source(j)
        remote(part.at[j], partr.at[here], qs.at[j], qr.at[here], zdev(1)).wait_recv()

    def combine(j):
        for d in range(1, npl):
            rcopy(j, d).wait_recv()
        rcopy(j, 0).wait()
        part[j] = tn(oh[j], rowr[j]).astype(jnp.bfloat16)
        if j:
            qcopy(j).start()

    tile = min(512, xe.shape[1])

    def grads(which):
        left, right, out = ((dat, xe, gg), (dbt, xe, gu), (ht, ge, gd))[which]

        @pl.loop(0, xe.shape[1] // tile)
        def _(t):
            here = pl.ds(pl.multiple_of(t * tile, tile), tile)
            out[0, :, here] = nn(left[...], right[:, here]).astype(jnp.bfloat16)

    last = nz - 1
    send_x(0)
    send_c(0)
    forward(0, 0)
    for i in range(1, nz):
        early(0, i)
        send_x(i)
        if i == 1:
            weights[0].wait()
            weights[1].wait()
        up(i - 1)
        forward(1, i - 1)
        early(1, i)
        send_c(i)
        if i == 1:
            weights[2].wait()
        if i == last:
            for j in range(1, last - 1):
                back(j)
        down(i - 1)
        forward(0, i)
    if nz == 1:
        for copy in weights:
            copy.wait()
    if last > 1:
        back(last - 1)
    up(last)
    forward(1, last)
    down(last)
    if last:
        back(last)
    for j in range(1, last - 1):
        combine(j)
    grads(0)
    if last > 1:
        combine(last - 1)
    back(0)
    grads(1)
    if last:
        combine(last)
    grads(2)
    combine(0)

    total = part[0].astype(jnp.float32)
    for j in range(1, nz):
        qwait(j)
        total = total + partr[source(j)].astype(jnp.float32)
    ig[...] = total.astype(jnp.bfloat16)
    if nz > 1:
        for kind in range(4):
            zfirst(kind, 1).wait_send()

            @pl.when(inner)
            def _():
                zfirst(kind, -1).wait_send()

        for k in range(1, nz):
            for holds, off, side in relays(k):

                @pl.when(holds)
                def _():
                    for kind in range(4):
                        zsend(kind, w + off, w + side).wait_send()

    for j in range(nz):
        if j:
            qcopy(j).wait_send()
        for d in range(1, npl):
            pcopy(0, j, d).wait_send()
            pcopy(1, j, d).wait_send()
            rcopy(j, d).wait_send()
        for d in range(1, ntp):
            for q in range(npl):
                tcopy(0, j, d, q, c).wait_send()
                tcopy(1, j, d, q, c).wait_send()
            dcopy(j, d).wait_send()


def finish(ig, gg, gu, gd, ig_hbm, gg_hbm, gu_hbm, gd_hbm, sem):
    copies = [
        pltpu.make_async_copy(v, h, sem.at[i])
        for i, (v, h) in enumerate(
            ((gg, gg_hbm), (gu, gu_hbm), (gd, gd_hbm), (ig, ig_hbm))
        )
    ]
    for copy in copies:
        copy.start()
    for copy in copies:
        copy.wait()


def local(nep, ntp, tokens, cotangent, expert_ids, gate_values, w_gate, w_up, w_down):
    tok_count, top = expert_ids.shape
    cap = max(2, tok_count * top * 4 // (nep * 3))
    nz = outer_factor(nep)
    npl = nep // nz
    width = tokens.shape[1]
    full = width * ntp
    hidden = w_gate.shape[1]
    batch = npl * cap
    count = nep * cap
    bf, f32 = jnp.bfloat16, jnp.float32
    vm = pltpu.VMEM
    dma = pltpu.SemaphoreType.DMA
    scratch = [
        vm((tok_count, width), bf), vm((tok_count, width), bf),
        vm((top, tok_count), jnp.int32), vm((top, tok_count), f32),
        vm((nz, tok_count, width), bf), vm((nz, tok_count, width), bf),
        vm((nz, top, tok_count), jnp.int32), vm((nz, top, tok_count), f32),
        vm((nz, batch, tok_count), bf), vm((nz, batch, 1), f32),
        vm((nz, batch, width), bf), vm((nz, batch, width), bf),
        vm((count, full), bf), vm((count, full), bf),
        vm((hidden, full), bf), vm((hidden, full), bf), vm((hidden, full), bf),
        vm((hidden, count), f32), vm((hidden, count), f32),
        vm((hidden, count), bf), vm((hidden, count), bf), vm((hidden, count), bf),
        vm((nz, batch, full), bf), vm((nz, ntp, batch, width), bf),
        vm((nz, batch, width), bf), vm((nz, batch, width), bf),
        vm((nz, tok_count, width), bf), vm((nz, tok_count, width), bf),
        dma((4,)), dma((3,)),
        dma((4, nz + 1)), dma((4, nz)),
        dma((2, nz, npl)), dma((2, nz, npl)), dma((2, nz)),
        dma((2, nz, npl, ntp)), dma((2, nz, npl, ntp)),
        dma((nz, ntp)), dma((nz, ntp)),
        dma((nz, npl)), dma((nz, npl)), dma((nz,)),
        dma((nz,)), dma((nz,)),
    ]
    inside = pl.BlockSpec(memory_space=pltpu.VMEM)
    outside = pl.BlockSpec(memory_space=pl.ANY)
    shapes = [tokens.shape, w_gate.shape, w_up.shape, w_down.shape]
    held = pl.pallas_call(
        functools.partial(kernel, nz, npl, ntp, cap),
        out_shape=tuple(vm(shape, bf) for shape in shapes),
        in_specs=[outside] * 7,
        out_specs=(inside,) * 4,
        scratch_shapes=scratch,
        compiler_params=pltpu.CompilerParams(
            collective_id=0, has_side_effects=True, vmem_limit_bytes=50 * 1024 * 1024
        ),
    )(tokens, cotangent, expert_ids.T, gate_values.T, w_gate, w_up, w_down)
    return pl.pallas_call(
        finish,
        out_shape=tuple(jax.ShapeDtypeStruct(shape, bf) for shape in shapes),
        in_specs=[inside] * 4,
        out_specs=(outside,) * 4,
        scratch_shapes=[dma((4,))],
        compiler_params=pltpu.CompilerParams(vmem_limit_bytes=1024 * 1024),
    )(*(pltpu.with_memory_space_constraint(value, pltpu.MemorySpace.VMEM) for value in held))


def solution(mesh):
    in_specs = (
        P("ep", "tp"), P("ep", "tp"), P("ep", None), P("ep", None),
        P("ep", "tp", None), P("ep", "tp", None), P("ep", "tp", None),
    )
    out_specs = (P("ep", "tp"), P("ep", "tp", None), P("ep", "tp", None), P("ep", "tp", None))
    body = functools.partial(local, mesh.shape["ep"], mesh.shape["tp"])
    return jax.shard_map(body, mesh=mesh, in_specs=in_specs, out_specs=out_specs, check_vma=False)
```

```python
import functools
import jax
import jax.numpy as jnp
from jax import lax
from jax.experimental import pallas as pl
from jax.experimental.pallas import tpu as pltpu
from jax.sharding import PartitionSpec as P


def outer_factor(count):
    outer = 1
    while outer * 2 * outer * 2 <= count and count % (outer * 2) == 0:
        outer *= 2
    return outer


def nt(left, right):
    return lax.dot_general(
        left, right, (((1,), (1,)), ((), ())), preferred_element_type=jnp.float32
    )


def tn(left, right):
    return lax.dot_general(
        left, right, (((0,), (0,)), ((), ())), preferred_element_type=jnp.float32
    )


def nn(left, right):
    return jnp.dot(left, right, preferred_element_type=jnp.float32)


def kernel(
    nz, npl, ntp, cap,
    tok_hbm, cot_hbm, ids_hbm, gat_hbm, wg_hbm, wu_hbm, wd_hbm,
    ig, gg, gu, gd,
    tok, cot, ids, gat, zx, zc, zi, zg,
    oh, grow, sx, sc, xe, ge, wg, wu, wd, at, bt, ht, dat, dbt,
    red, redr, rows, rowr, part, partr, near, seen, home, homer, acc,
    s_i, s_w, zs, zr, ps, pr, ls, ts, tr, ds, dr, rs, rr, rl, qs, qr, ns, nr, es, er, hs, hr,
):
    ep = lax.axis_index("ep")
    c = lax.axis_index("tp")
    z = ep // npl
    p = ep % npl
    width = tok.shape[1]
    batch = npl * cap
    half = max(1, nz // 2)
    upper = z // half if nz > 1 else 0
    w = z + upper * (nz - 1 - 2 * z)
    inner = w > 0

    def mirror(v):
        return v + upper * (nz - 1 - 2 * v)

    def source(i):
        d = (i + 1) // 2
        near_ = (w - d + nz) // nz
        return mirror(near_ * (w + (d if i % 2 else -d)) + (1 - near_) * i)

    def zdev(j):
        return {"ep": ((z + j) % nz) * npl + p}

    def pdev(d):
        return {"ep": z * npl + (p + d) % npl}

    def tdev(d):
        return {"tp": (c + d) % ntp}

    def cols(core):
        return pl.ds(pl.multiple_of(core * width, width), width)

    def remote(src, dst, ssem, rsem, dev):
        return pltpu.make_async_remote_copy(
            src_ref=src, dst_ref=dst, send_sem=ssem, recv_sem=rsem,
            device_id=dev, device_id_type=pl.DeviceIdType.MESH,
        )

    inputs = [
        pltpu.make_async_copy(h, v, s_i.at[i])
        for i, (h, v) in enumerate(
            ((ids_hbm, ids), (gat_hbm, gat), (tok_hbm, tok), (cot_hbm, cot))
        )
    ]
    for copy in inputs:
        copy.start()

    barrier = pltpu.get_barrier_semaphore()
    peers = [{"ep": mirror(w + 1) * npl + p}] if nz > 1 else []
    peers += [pdev(d) for d in range(1, npl)]
    peers += [tdev(d) for d in range(1, ntp)]

    def greet(dev):
        pl.semaphore_signal(barrier, inc=1, device_id=dev, device_id_type=pl.DeviceIdType.MESH)

    for dev in peers:
        greet(dev)
    if nz > 1:

        @pl.when(inner)
        def _():
            greet({"ep": mirror(w - 1) * npl + p})

    zown = (ids, gat, tok, cot)
    zin = (zi, zg, zx, zc)

    def zsend(kind, block, to):
        slot = mirror(block)
        return remote(
            zin[kind].at[slot], zin[kind].at[slot], zs.at[kind, slot], zr.at[kind, slot],
            {"ep": mirror(to) * npl + p},
        )

    def zfirst(kind, side):
        sem = zs.at[kind, z if side > 0 else nz]
        return remote(
            zown[kind], zin[kind].at[z], sem, zr.at[kind, z], {"ep": mirror(w + side) * npl + p}
        )

    def relays(k):
        found = []
        if k < nz:
            found.append((inner if k <= nz - half else inner & (w + k < nz), k, -1))
        if k < half:
            found.append((w >= k, -k, 1))
        return found

    def kinds(kind):
        return (0, 1, 2) if kind == 0 else (3,)

    def early(kind, k):
        for holds, off, side in relays(k):

            @pl.when(holds)
            def _():
                for part_ in kinds(kind):
                    copy = zsend(part_, w + off, w + side)
                    copy.wait_recv()
                    copy.start()

    def late(kind, i):
        @pl.when(w == 0)
        def _():
            for part_ in kinds(kind):
                zsend(part_, i, w).wait_recv()

    ntok = ids.shape[1]
    before = (
        lax.broadcasted_iota(jnp.int32, (ntok, ntok), 0)
        < lax.broadcasted_iota(jnp.int32, (ntok, ntok), 1)
    ).astype(jnp.bfloat16)
    slot_iota = lax.broadcasted_iota(jnp.int32, (cap, ntok), 0).astype(jnp.float32)

    def pall(kind, j):
        view = (sx, sc)[kind].at[j, pl.ds(cap, batch - cap), :]
        return remote(view, view, ps.at[kind, j], pr.at[kind, j, 0], pdev(1 % npl))

    def choose(named, e):
        hit = named == e
        has = jnp.sum(jnp.where(hit, 1.0, 0.0), axis=0, keepdims=True)
        pos = nn(jnp.broadcast_to(has, (16, ntok)).astype(jnp.bfloat16), before)[0:1]
        return hit, jnp.where(slot_iota == pos, 1.0, 0.0) * has

    def build(j):
        named = ids[...] if j == 0 else zi[source(j)]
        gates = gat[...] if j == 0 else zg[source(j)]
        for d in range(npl):
            hit, sel = choose(named, z * npl + (p + d) % npl)
            gate = jnp.sum(jnp.where(hit, gates, 0.0), axis=0, keepdims=True)
            oh[j, d * cap:(d + 1) * cap, :] = sel.astype(jnp.bfloat16)
            grow[j, d * cap:(d + 1) * cap, :] = jnp.sum(sel * gate, axis=1, keepdims=True)

    def pcopy(kind, j, d):
        src, dst = ((sx, xe), (sc, ge))[kind]
        lines = pl.ds(j * batch + d * cap, cap)
        s, t = src.at[j, pl.ds(d * cap, cap), :], dst.at[lines, cols(c)]
        if d == 0:
            return pltpu.make_async_copy(s, t, ls.at[kind, j])
        return remote(s, t, ps.at[kind, j], pr.at[kind, j, d - 1], pdev(d))

    def pick_x(j):
        build(j)
        block = tok[...] if j == 0 else zx[source(j)]
        sx[j] = nn(oh[j], block).astype(jnp.bfloat16)

    def pick_c(j):
        block = cot[...] if j == 0 else zc[source(j)]
        sc[j] = (nn(oh[j], block) * grow[j]).astype(jnp.bfloat16)

    def spread(kind, j):
        for d in range(1, npl):
            pcopy(kind, j, d).start()
        pcopy(kind, j, 0).start()

    def send_x(j):
        late(0, j)
        pick_x(j)
        spread(0, j)

    def send_c(j):
        late(1, j)
        pick_c(j)
        spread(1, j)

    def tcopy(kind, j, d, q, count, owner):
        buf = (xe, ge)[kind]
        view = buf.at[pl.ds(j * batch + q * cap, count * cap), cols(owner)]
        return remote(view, view, ts.at[kind, j, d - 1], tr.at[kind, j, d - 1], tdev(d))

    def forward(kind, j):
        for q in range(npl):
            if q:
                pcopy(kind, j, q).wait_recv()
            else:
                pcopy(kind, j, 0).wait()
            for d in range(1, ntp):
                tcopy(kind, j, d, q, 1, c).start()

    def arrive(kind, j):
        for d in range(1, ntp):
            tcopy(kind, j, d, 0, npl, (c + ntp - d) % ntp).wait_recv()

    def up(j):
        arrive(0, j)
        x = xe[j * batch:(j + 1) * batch, :]
        at[:, j * batch:(j + 1) * batch] = nt(wg[...], x)
        bt[:, j * batch:(j + 1) * batch] = nt(wu[...], x)

    def dcopy(j, d):
        return remote(
            red.at[j, :, cols((c + d) % ntp)], redr.at[j, d - 1],
            ds.at[j, d - 1], dr.at[j, d - 1], tdev(d),
        )

    def down(j):
        arrive(1, j)
        lines = slice(j * batch, (j + 1) * batch)
        dh = nt(wd[...], ge[lines, :])
        a, b = at[:, lines], bt[:, lines]
        s = jax.nn.sigmoid(a)
        swish = a * s
        ht[:, lines] = (swish * b).astype(jnp.bfloat16)
        da = (dh * b * s * (1.0 + a * (1.0 - s))).astype(jnp.bfloat16)
        db = (dh * swish).astype(jnp.bfloat16)
        dat[:, lines] = da
        dbt[:, lines] = db
        for d in [*range(1, ntp), 0]:
            here = cols((c + d) % ntp)
            red[j, :, here] = (tn(da, wg[:, here]) + tn(db, wu[:, here])).astype(jnp.bfloat16)
            if d:
                dcopy(j, d).start()

    def rcopy(j, d):
        lines = pl.ds(d * cap, cap)
        s, t = rows.at[j, lines, :], rowr.at[j, lines, :]
        if d == 0:
            return pltpu.make_async_copy(s, t, rl.at[j])
        return remote(s, t, rs.at[j], rr.at[j], pdev(npl - d))

    def rall(j):
        lines = pl.ds(cap, batch - cap)
        return remote(
            rows.at[j, lines, :], rowr.at[j, lines, :], rs.at[j], rr.at[j], pdev(1 % npl)
        )

    def gather(j):
        total = red[j, :, cols(c)].astype(jnp.float32)
        for d in range(1, ntp):
            dcopy(j, d).wait_recv()
            total = total + redr[j, d - 1].astype(jnp.float32)
        rows[j] = total.astype(jnp.bfloat16)

    def back(j):
        gather(j)
        for d in range(1, npl):
            rcopy(j, d).start()
        rcopy(j, 0).start()

    def ncopy(slot, to):
        return remote(
            rows.at[1], near.at[slot], ns.at[0], nr.at[slot], {"ep": mirror(to) * npl + p}
        )

    def hand():
        gather(1)

        @pl.when(w < half - 1)
        def _():
            ncopy(0, w + 1).start()

        @pl.when(w == half - 1)
        def _():
            ncopy(1, w + 1).start()

    def ecopy(d):
        return remote(ids, seen.at[d], es.at[0], er.at[0], pdev(d))

    def eall():
        view = seen.at[pl.ds(1, npl - 1)]
        return remote(view, view, es.at[0], er.at[0], pdev(1 % npl))

    def hcopy(d):
        return remote(home.at[d], homer.at[d], hs.at[0], hr.at[0], pdev(npl - d))

    def hall():
        some = pl.ds(1, npl - 1)
        return remote(home.at[some], homer.at[some], hs.at[0], hr.at[0], pdev(1 % npl))

    def fold(slot, holds, block):
        @pl.when(holds)
        def _():
            ncopy(slot, w + 1).wait_recv()
            for d in range(npl):
                named = ids[...] if d == 0 else seen[d]
                sel = choose(named, mirror(block) * npl + p)[1].astype(jnp.bfloat16)
                acc[d] += tn(sel, near[slot, d * cap:(d + 1) * cap, :])

    def homeward():
        gather(0)
        if npl > 1:
            eall().wait_recv()
        for d in range(npl):
            named = ids[...] if d == 0 else seen[d]
            sel = choose(named, z * npl + p)[1].astype(jnp.bfloat16)
            acc[d] = tn(sel, rows[0, d * cap:(d + 1) * cap, :])
        if nz > 1:
            fold(0, inner, w - 1)
            fold(1, w == half - 1, w + 1)
        for d in range(npl):
            home[d] = acc[d].astype(jnp.bfloat16)
            if d:
                hcopy(d).start()

    def qcopy(j):
        return remote(
            part.at[j], partr.at[z], qs.at[j], qr.at[z], {"ep": source(j) * npl + p}
        )

    def qwait(j):
        here = source(j)
        remote(part.at[j], partr.at[here], qs.at[j], qr.at[here], zdev(1)).wait_recv()

    def combine(j):
        if npl > 1:
            rall(j).wait_recv()
        rcopy(j, 0).wait()
        part[j] = tn(oh[j], rowr[j]).astype(jnp.bfloat16)
        if j:
            qcopy(j).start()

    tile = min(512, xe.shape[1])

    def grads(which):
        left, right, out = ((dat, xe, gg), (dbt, xe, gu), (ht, ge, gd))[which]

        @pl.loop(0, xe.shape[1] // tile)
        def _(t):
            here = pl.ds(pl.multiple_of(t * tile, tile), tile)
            out[0, :, here] = nn(left[...], right[:, here]).astype(jnp.bfloat16)

    last = nz - 1
    for copy in inputs[:3]:
        copy.wait()
    pick_x(0)
    inputs[3].wait()
    pick_c(0)
    pl.semaphore_wait(barrier, len(peers) + (w + nz - 1) // nz)
    for kind in range(4):
        if nz > 1:
            zfirst(kind, 1).start()

            @pl.when(inner)
            def _():
                zfirst(kind, -1).start()

    weights = [
        pltpu.make_async_copy(h.at[0], v, s_w.at[i])
        for i, (h, v) in enumerate(((wg_hbm, wg), (wu_hbm, wu), (wd_hbm, wd)))
    ]
    for copy in weights:
        copy.start()

    spread(0, 0)
    for d in range(1, npl):
        ecopy(d).start()
    spread(1, 0)
    forward(0, 0)
    for i in range(1, nz):
        early(0, i)
        send_x(i)
        if i == 1:
            weights[0].wait()
            weights[1].wait()
        if i == 3:
            hand()
        up(i - 1)
        forward(1, i - 1)
        early(1, i)
        send_c(i)
        if i == 1:
            weights[2].wait()
        if i == last:
            for j in range(2, last - 1):
                back(j)
        down(i - 1)
        forward(0, i)
    if nz == 1:
        for copy in weights:
            copy.wait()
    if last == 2:
        hand()
    if last > 2:
        back(last - 1)
    up(last)
    forward(1, last)
    down(last)
    for j in range(2, last):
        combine(j)
    if last > 1:
        back(last)
    if last == 1:
        hand()
    homeward()
    grads(0)
    if last > 1:
        combine(last)
    grads(1)
    grads(2)

    acc[0] = home[0].astype(jnp.float32)
    if npl > 1:
        hall().wait_recv()
    for d in range(1, npl):
        acc[0] += homer[d].astype(jnp.float32)
    for j in range(2, nz):

        @pl.when(w == 0 if j == 2 else w >= 0)
        def _():
            qwait(j)
            acc[0] += partr[source(j)].astype(jnp.float32)

    if nz > 1:

        @pl.when(w < half - 1)
        def _():
            qwait(1)
            acc[0] += partr[source(1)].astype(jnp.float32)

    ig[...] = acc[0].astype(jnp.bfloat16)
    if nz > 1:
        for kind in range(4):
            zfirst(kind, 1).wait_send()

            @pl.when(inner)
            def _():
                zfirst(kind, -1).wait_send()

        for k in range(1, nz):
            for holds, off, side in relays(k):

                @pl.when(holds)
                def _():
                    for kind in range(4):
                        zsend(kind, w + off, w + side).wait_send()

    if nz > 1:
        ncopy(0, w + 1).wait_send()
    if npl > 1:
        eall().wait_send()
        hall().wait_send()
    for j in range(nz):
        if j > 1:
            qcopy(j).wait_send()
        if npl > 1:
            pall(0, j).wait_send()
            pall(1, j).wait_send()
            if j > 1:
                rall(j).wait_send()
        for d in range(1, ntp):
            tcopy(0, j, d, 0, npl, c).wait_send()
            tcopy(1, j, d, 0, npl, c).wait_send()
            dcopy(j, d).wait_send()


def finish(ig, gg, gu, gd, ig_hbm, gg_hbm, gu_hbm, gd_hbm, sem):
    copies = [
        pltpu.make_async_copy(v, h, sem.at[i])
        for i, (v, h) in enumerate(
            ((gg, gg_hbm), (gu, gu_hbm), (gd, gd_hbm), (ig, ig_hbm))
        )
    ]
    for copy in copies:
        copy.start()
    for copy in copies:
        copy.wait()


def local(nep, ntp, tokens, cotangent, expert_ids, gate_values, w_gate, w_up, w_down):
    tok_count, top = expert_ids.shape
    cap = max(2, tok_count * top * 4 // (nep * 3))
    nz = outer_factor(nep)
    npl = nep // nz
    width = tokens.shape[1]
    full = width * ntp
    hidden = w_gate.shape[1]
    batch = npl * cap
    count = nep * cap
    bf, f32 = jnp.bfloat16, jnp.float32
    vm = pltpu.VMEM
    dma = pltpu.SemaphoreType.DMA
    scratch = [
        vm((tok_count, width), bf), vm((tok_count, width), bf),
        vm((top, tok_count), jnp.int32), vm((top, tok_count), f32),
        vm((nz, tok_count, width), bf), vm((nz, tok_count, width), bf),
        vm((nz, top, tok_count), jnp.int32), vm((nz, top, tok_count), f32),
        vm((nz, batch, tok_count), bf), vm((nz, batch, 1), f32),
        vm((nz, batch, width), bf), vm((nz, batch, width), bf),
        vm((count, full), bf), vm((count, full), bf),
        vm((hidden, full), bf), vm((hidden, full), bf), vm((hidden, full), bf),
        vm((hidden, count), f32), vm((hidden, count), f32),
        vm((hidden, count), bf), vm((hidden, count), bf), vm((hidden, count), bf),
        vm((nz, batch, full), bf), vm((nz, max(1, ntp - 1), batch, width), bf),
        vm((nz, batch, width), bf), vm((nz, batch, width), bf),
        vm((nz, tok_count, width), bf), vm((nz, tok_count, width), bf),
        vm((2, batch, width), bf), vm((npl, top, tok_count), jnp.int32),
        vm((npl, tok_count, width), bf), vm((npl, tok_count, width), bf),
        vm((npl, tok_count, width), f32),
        dma((4,)), dma((3,)),
        dma((4, nz + 1)), dma((4, nz)),
        dma((2, nz)), dma((2, nz, max(1, npl - 1))), dma((2, nz)),
        dma((2, nz, max(1, ntp - 1))), dma((2, nz, max(1, ntp - 1))),
        dma((nz, max(1, ntp - 1))), dma((nz, max(1, ntp - 1))),
        dma((nz,)), dma((nz,)), dma((nz,)),
        dma((nz,)), dma((nz,)), dma((1,)), dma((2,)),
        dma((1,)), dma((1,)), dma((1,)), dma((1,)),
    ]
    inside = pl.BlockSpec(memory_space=pltpu.VMEM)
    outside = pl.BlockSpec(memory_space=pl.ANY)
    shapes = [tokens.shape, w_gate.shape, w_up.shape, w_down.shape]
    held = pl.pallas_call(
        functools.partial(kernel, nz, npl, ntp, cap),
        out_shape=tuple(vm(shape, bf) for shape in shapes),
        in_specs=[outside] * 7,
        out_specs=(inside,) * 4,
        scratch_shapes=scratch,
        compiler_params=pltpu.CompilerParams(
            collective_id=0, has_side_effects=True, vmem_limit_bytes=53 * 1024 * 1024
        ),
    )(tokens, cotangent, expert_ids.T, gate_values.T, w_gate, w_up, w_down)
    return pl.pallas_call(
        finish,
        out_shape=tuple(jax.ShapeDtypeStruct(shape, bf) for shape in shapes),
        in_specs=[inside] * 4,
        out_specs=(outside,) * 4,
        scratch_shapes=[dma((4,))],
        compiler_params=pltpu.CompilerParams(vmem_limit_bytes=1024 * 1024),
    )(*(pltpu.with_memory_space_constraint(value, pltpu.MemorySpace.VMEM) for value in held))


def solution(mesh):
    in_specs = (
        P("ep", "tp"), P("ep", "tp"), P("ep", None), P("ep", None),
        P("ep", "tp", None), P("ep", "tp", None), P("ep", "tp", None),
    )
    out_specs = (P("ep", "tp"), P("ep", "tp", None), P("ep", "tp", None), P("ep", "tp", None))
    body = functools.partial(local, mesh.shape["ep"], mesh.shape["tp"])
    return jax.shard_map(body, mesh=mesh, in_specs=in_specs, out_specs=out_specs, check_vma=False)
```

```python
import functools
import jax
import jax.numpy as jnp
from jax import lax
from jax.experimental import pallas as pl
from jax.experimental.pallas import tpu as pltpu
from jax.sharding import PartitionSpec as P


def outer_factor(count):
    outer = 1
    while outer * 2 * outer * 2 <= count and count % (outer * 2) == 0:
        outer *= 2
    return outer


def nt(left, right):
    return lax.dot_general(
        left, right, (((1,), (1,)), ((), ())), preferred_element_type=jnp.float32
    )


def tn(left, right):
    return lax.dot_general(
        left, right, (((0,), (0,)), ((), ())), preferred_element_type=jnp.float32
    )


def nn(left, right):
    return jnp.dot(left, right, preferred_element_type=jnp.float32)


def kernel(
    nz, npl, ntp, cap,
    tok_hbm, cot_hbm, ids_hbm, gat_hbm, wg_hbm, wu_hbm, wd_hbm,
    ig, gg, gu, gd,
    tok, cot, ids, gat, zx, zc, zi, zg,
    oh, grow, sx, sc, xe, ge, wg, wu, wd, at, bt, ht, dat, dbt,
    red, redr, rows, rowr, part, partr, near, seen, home, homer, acc,
    s_i, s_w, zs, zr, ps, pr, ls, ts, tr, ds, dr, rs, rr, rl, qs, qr, ns, nr, es, er, hs, hr,
):
    ep = lax.axis_index("ep")
    c = lax.axis_index("tp")
    z = ep // npl
    p = ep % npl
    width = tok.shape[1]
    batch = npl * cap
    half = max(1, nz // 2)
    upper = z // half if nz > 1 else 0
    w = z + upper * (nz - 1 - 2 * z)
    inner = w > 0

    def mirror(v):
        return v + upper * (nz - 1 - 2 * v)

    def source(i):
        d = (i + 1) // 2
        near_ = (w - d + nz) // nz
        return mirror(near_ * (w + (d if i % 2 else -d)) + (1 - near_) * i)

    def zdev(j):
        return {"ep": ((z + j) % nz) * npl + p}

    def pdev(d):
        return {"ep": z * npl + (p + d) % npl}

    def tdev(d):
        return {"tp": (c + d) % ntp}

    def cols(core):
        return pl.ds(pl.multiple_of(core * width, width), width)

    def remote(src, dst, ssem, rsem, dev):
        return pltpu.make_async_remote_copy(
            src_ref=src, dst_ref=dst, send_sem=ssem, recv_sem=rsem,
            device_id=dev, device_id_type=pl.DeviceIdType.MESH,
        )

    inputs = [
        pltpu.make_async_copy(h, v, s_i.at[i])
        for i, (h, v) in enumerate(
            ((ids_hbm, ids), (gat_hbm, gat), (tok_hbm, tok), (cot_hbm, cot))
        )
    ]
    for copy in inputs:
        copy.start()

    barrier = pltpu.get_barrier_semaphore()
    peers = [{"ep": mirror(w + 1) * npl + p}] if nz > 1 else []
    peers += [pdev(d) for d in range(1, npl)]
    peers += [tdev(d) for d in range(1, ntp)]

    def greet(dev):
        pl.semaphore_signal(barrier, inc=1, device_id=dev, device_id_type=pl.DeviceIdType.MESH)

    for dev in peers:
        greet(dev)
    if nz > 1:

        @pl.when(inner)
        def _():
            greet({"ep": mirror(w - 1) * npl + p})

    zown = (ids, gat, tok, cot)
    zin = (zi, zg, zx, zc)

    def zsend(kind, block, to):
        slot = mirror(block)
        return remote(
            zin[kind].at[slot], zin[kind].at[slot], zs.at[kind, slot], zr.at[kind, slot],
            {"ep": mirror(to) * npl + p},
        )

    def zfirst(kind, side):
        sem = zs.at[kind, z if side > 0 else nz]
        return remote(
            zown[kind], zin[kind].at[z], sem, zr.at[kind, z], {"ep": mirror(w + side) * npl + p}
        )

    def relays(k):
        found = []
        if k < nz:
            found.append((inner if k <= nz - half else inner & (w + k < nz), k, -1))
        if k < half:
            found.append((w >= k, -k, 1))
        return found

    def kinds(kind):
        return (0, 1, 2) if kind == 0 else (3,)

    def early(kind, k):
        for holds, off, side in relays(k):

            @pl.when(holds)
            def _():
                for part_ in kinds(kind):
                    copy = zsend(part_, w + off, w + side)
                    copy.wait_recv()
                    copy.start()

    def late(kind, i):
        @pl.when(w == 0)
        def _():
            for part_ in kinds(kind):
                zsend(part_, i, w).wait_recv()

    ntok = ids.shape[1]
    before = (
        lax.broadcasted_iota(jnp.int32, (ntok, ntok), 0)
        < lax.broadcasted_iota(jnp.int32, (ntok, ntok), 1)
    ).astype(jnp.bfloat16)
    slot_iota = lax.broadcasted_iota(jnp.int32, (cap, ntok), 0).astype(jnp.float32)

    def pall(kind, j):
        view = (sx, sc)[kind].at[j, pl.ds(cap, batch - cap), :]
        return remote(view, view, ps.at[kind, j], pr.at[kind, j, 0], pdev(1 % npl))

    def choose(named, e):
        hit = named == e
        has = jnp.sum(jnp.where(hit, 1.0, 0.0), axis=0, keepdims=True)
        pos = nn(jnp.broadcast_to(has, (16, ntok)).astype(jnp.bfloat16), before)[0:1]
        return hit, jnp.where(slot_iota == pos, 1.0, 0.0) * has

    def build(j):
        named = ids[...] if j == 0 else zi[source(j)]
        gates = gat[...] if j == 0 else zg[source(j)]
        for d in range(npl):
            hit, sel = choose(named, z * npl + (p + d) % npl)
            gate = jnp.sum(jnp.where(hit, gates, 0.0), axis=0, keepdims=True)
            oh[j, d * cap:(d + 1) * cap, :] = sel.astype(jnp.bfloat16)
            grow[j, d * cap:(d + 1) * cap, :] = jnp.sum(sel * gate, axis=1, keepdims=True)

    def pcopy(kind, j, d):
        src, dst = ((sx, xe), (sc, ge))[kind]
        lines = pl.ds(j * batch + d * cap, cap)
        s, t = src.at[j, pl.ds(d * cap, cap), :], dst.at[lines, cols(c)]
        if d == 0:
            return pltpu.make_async_copy(s, t, ls.at[kind, j])
        return remote(s, t, ps.at[kind, j], pr.at[kind, j, d - 1], pdev(d))

    def pick_x(j):
        build(j)
        block = tok[...] if j == 0 else zx[source(j)]
        sx[j] = nn(oh[j], block).astype(jnp.bfloat16)

    def pick_c(j):
        block = cot[...] if j == 0 else zc[source(j)]
        sc[j] = (nn(oh[j], block) * grow[j]).astype(jnp.bfloat16)

    def spread(kind, j):
        for d in range(1, npl):
            pcopy(kind, j, d).start()
        pcopy(kind, j, 0).start()

    def send_x(j):
        late(0, j)
        pick_x(j)
        spread(0, j)

    def send_c(j):
        late(1, j)
        pick_c(j)
        spread(1, j)

    def tcopy(kind, j, d, q, count, owner):
        buf = (xe, ge)[kind]
        view = buf.at[pl.ds(j * batch + q * cap, count * cap), cols(owner)]
        return remote(view, view, ts.at[kind, j, d - 1], tr.at[kind, j, d - 1], tdev(d))

    def forward(kind, j):
        for q in range(npl):
            if q:
                pcopy(kind, j, q).wait_recv()
            else:
                pcopy(kind, j, 0).wait()
            for d in range(1, ntp):
                tcopy(kind, j, d, q, 1, c).start()

    def arrive(kind, j):
        for d in range(1, ntp):
            tcopy(kind, j, d, 0, npl, (c + ntp - d) % ntp).wait_recv()

    def up(j):
        arrive(0, j)
        x = xe[j * batch:(j + 1) * batch, :]
        at[:, j * batch:(j + 1) * batch] = nt(wg[...], x)
        bt[:, j * batch:(j + 1) * batch] = nt(wu[...], x)

    def dcopy(j, d):
        return remote(
            red.at[j, :, cols((c + d) % ntp)], redr.at[j, d - 1],
            ds.at[j, d - 1], dr.at[j, d - 1], tdev(d),
        )

    def down(j):
        arrive(1, j)
        lines = slice(j * batch, (j + 1) * batch)
        dh = nt(wd[...], ge[lines, :])
        a, b = at[:, lines], bt[:, lines]
        s = jax.nn.sigmoid(a)
        swish = a * s
        ht[:, lines] = (swish * b).astype(jnp.bfloat16)
        da = (dh * b * s * (1.0 + a * (1.0 - s))).astype(jnp.bfloat16)
        db = (dh * swish).astype(jnp.bfloat16)
        dat[:, lines] = da
        dbt[:, lines] = db
        for d in [*range(1, ntp), 0]:
            here = cols((c + d) % ntp)
            red[j, :, here] = (tn(da, wg[:, here]) + tn(db, wu[:, here])).astype(jnp.bfloat16)
            if d:
                dcopy(j, d).start()

    wide = width // 2

    def strip(h):
        return pl.ds(h * wide, wide)

    def rcopy(j, d, h):
        lines = pl.ds(d * cap, cap)
        s, t = rows.at[j, lines, strip(h)], rowr.at[j, lines, strip(h)]
        if d == 0:
            return pltpu.make_async_copy(s, t, rl.at[j, h])
        return remote(s, t, rs.at[j, h], rr.at[j, h], pdev(npl - d))

    def rall(j, h):
        lines = pl.ds(cap, batch - cap)
        return remote(
            rows.at[j, lines, strip(h)], rowr.at[j, lines, strip(h)],
            rs.at[j, h], rr.at[j, h], pdev(1 % npl),
        )

    def gather(j):
        total = red[j, :, cols(c)].astype(jnp.float32)
        for d in range(1, ntp):
            dcopy(j, d).wait_recv()
            total = total + redr[j, d - 1].astype(jnp.float32)
        rows[j] = total.astype(jnp.bfloat16)

    def back(j):
        gather(j)
        for h in range(2):
            for d in range(1, npl):
                rcopy(j, d, h).start()
            rcopy(j, 0, h).start()

    def ncopy(slot, to):
        return remote(
            rows.at[1], near.at[slot], ns.at[0], nr.at[slot], {"ep": mirror(to) * npl + p}
        )

    def hand():
        gather(1)

        @pl.when(w < half - 1)
        def _():
            ncopy(0, w + 1).start()

        @pl.when(w == half - 1)
        def _():
            ncopy(1, w + 1).start()

    def ecopy(d):
        return remote(ids, seen.at[d], es.at[0], er.at[0], pdev(d))

    def eall():
        view = seen.at[pl.ds(1, npl - 1)]
        return remote(view, view, es.at[0], er.at[0], pdev(1 % npl))

    def hcopy(d):
        return remote(home.at[d], homer.at[d], hs.at[0], hr.at[0], pdev(npl - d))

    def hall():
        some = pl.ds(1, npl - 1)
        return remote(home.at[some], homer.at[some], hs.at[0], hr.at[0], pdev(1 % npl))

    def fold(slot, holds, block):
        @pl.when(holds)
        def _():
            ncopy(slot, w + 1).wait_recv()
            for d in range(npl):
                named = ids[...] if d == 0 else seen[d]
                sel = choose(named, mirror(block) * npl + p)[1].astype(jnp.bfloat16)
                acc[d] += tn(sel, near[slot, d * cap:(d + 1) * cap, :])

    def homeward():
        gather(0)
        if npl > 1:
            eall().wait_recv()
        for d in range(npl):
            named = ids[...] if d == 0 else seen[d]
            sel = choose(named, z * npl + p)[1].astype(jnp.bfloat16)
            acc[d] = tn(sel, rows[0, d * cap:(d + 1) * cap, :])
        if nz > 1:
            fold(0, inner, w - 1)
            fold(1, w == half - 1, w + 1)
        for d in range(npl):
            home[d] = acc[d].astype(jnp.bfloat16)

    def qcopy(j, h):
        return remote(
            part.at[j, :, strip(h)], partr.at[z, :, strip(h)], qs.at[j, h], qr.at[z, h],
            {"ep": source(j) * npl + p},
        )

    def qwait(j):
        here = source(j)
        for h in range(2):
            view = partr.at[here, :, strip(h)]
            remote(view, view, qs.at[j, h], qr.at[here, h], zdev(1)).wait_recv()

    def combine(j, h):
        if npl > 1:
            rall(j, h).wait_recv()
        rcopy(j, 0, h).wait()
        part[j, :, strip(h)] = tn(oh[j], rowr[j, :, strip(h)]).astype(jnp.bfloat16)
        qcopy(j, h).start()

    tile = min(512, xe.shape[1])

    def grads(which):
        left, right, out = ((dat, xe, gg), (dbt, xe, gu), (ht, ge, gd))[which]

        @pl.loop(0, xe.shape[1] // tile)
        def _(t):
            here = pl.ds(pl.multiple_of(t * tile, tile), tile)
            out[0, :, here] = nn(left[...], right[:, here]).astype(jnp.bfloat16)

    last = nz - 1
    for copy in inputs[:3]:
        copy.wait()
    pick_x(0)
    inputs[3].wait()
    pick_c(0)
    pl.semaphore_wait(barrier, len(peers) + (w + nz - 1) // nz)
    for kind in range(4):
        if nz > 1:
            zfirst(kind, 1).start()

            @pl.when(inner)
            def _():
                zfirst(kind, -1).start()

    weights = [
        pltpu.make_async_copy(h.at[0], v, s_w.at[i])
        for i, (h, v) in enumerate(((wg_hbm, wg), (wu_hbm, wu), (wd_hbm, wd)))
    ]
    for copy in weights:
        copy.start()

    spread(0, 0)
    for d in range(1, npl):
        ecopy(d).start()
    spread(1, 0)
    forward(0, 0)
    for i in range(1, nz):
        early(0, i)
        send_x(i)
        if i == 1:
            weights[0].wait()
            weights[1].wait()
        if i == 3:
            hand()
        up(i - 1)
        forward(1, i - 1)
        early(1, i)
        send_c(i)
        if i == 1:
            weights[2].wait()
        if i == last:
            for j in range(2, last - 1):
                back(j)
        down(i - 1)
        forward(0, i)
    if nz == 1:
        for copy in weights:
            copy.wait()
    if last == 2:
        hand()
    if last > 2:
        back(last - 1)
    up(last)
    forward(1, last)
    down(last)
    for j in range(2, last):
        combine(j, 0)
        combine(j, 1)
    if last > 1:
        back(last)
    if last == 1:
        hand()
    homeward()
    grads(0)
    if last > 1:
        combine(last, 0)
    for d in range(1, npl):
        hcopy(d).start()
    if last > 1:
        combine(last, 1)
    grads(1)
    grads(2)

    acc[0] = home[0].astype(jnp.float32)
    if npl > 1:
        hall().wait_recv()
    for d in range(1, npl):
        acc[0] += homer[d].astype(jnp.float32)
    for j in range(2, nz):

        @pl.when(w == 0 if j == 2 else w >= 0)
        def _():
            qwait(j)
            acc[0] += partr[source(j)].astype(jnp.float32)

    if nz > 1:

        @pl.when(w < half - 1)
        def _():
            qwait(1)
            acc[0] += partr[source(1)].astype(jnp.float32)

    ig[...] = acc[0].astype(jnp.bfloat16)
    if nz > 1:
        for kind in range(4):
            zfirst(kind, 1).wait_send()

            @pl.when(inner)
            def _():
                zfirst(kind, -1).wait_send()

        for k in range(1, nz):
            for holds, off, side in relays(k):

                @pl.when(holds)
                def _():
                    for kind in range(4):
                        zsend(kind, w + off, w + side).wait_send()

    if nz > 1:
        ncopy(0, w + 1).wait_send()
    if npl > 1:
        eall().wait_send()
        hall().wait_send()
    for j in range(nz):
        if j > 1:
            qcopy(j, 0).wait_send()
            qcopy(j, 1).wait_send()
        if npl > 1:
            pall(0, j).wait_send()
            pall(1, j).wait_send()
            if j > 1:
                rall(j, 0).wait_send()
                rall(j, 1).wait_send()
        for d in range(1, ntp):
            tcopy(0, j, d, 0, npl, c).wait_send()
            tcopy(1, j, d, 0, npl, c).wait_send()
            dcopy(j, d).wait_send()


def finish(ig, gg, gu, gd, ig_hbm, gg_hbm, gu_hbm, gd_hbm, sem):
    copies = [
        pltpu.make_async_copy(v, h, sem.at[i])
        for i, (v, h) in enumerate(
            ((gg, gg_hbm), (gu, gu_hbm), (gd, gd_hbm), (ig, ig_hbm))
        )
    ]
    for copy in copies:
        copy.start()
    for copy in copies:
        copy.wait()


def local(nep, ntp, tokens, cotangent, expert_ids, gate_values, w_gate, w_up, w_down):
    tok_count, top = expert_ids.shape
    cap = max(2, tok_count * top * 4 // (nep * 3))
    nz = outer_factor(nep)
    npl = nep // nz
    width = tokens.shape[1]
    full = width * ntp
    hidden = w_gate.shape[1]
    batch = npl * cap
    count = nep * cap
    bf, f32 = jnp.bfloat16, jnp.float32
    vm = pltpu.VMEM
    dma = pltpu.SemaphoreType.DMA
    scratch = [
        vm((tok_count, width), bf), vm((tok_count, width), bf),
        vm((top, tok_count), jnp.int32), vm((top, tok_count), f32),
        vm((nz, tok_count, width), bf), vm((nz, tok_count, width), bf),
        vm((nz, top, tok_count), jnp.int32), vm((nz, top, tok_count), f32),
        vm((nz, batch, tok_count), bf), vm((nz, batch, 1), f32),
        vm((nz, batch, width), bf), vm((nz, batch, width), bf),
        vm((count, full), bf), vm((count, full), bf),
        vm((hidden, full), bf), vm((hidden, full), bf), vm((hidden, full), bf),
        vm((hidden, count), f32), vm((hidden, count), f32),
        vm((hidden, count), bf), vm((hidden, count), bf), vm((hidden, count), bf),
        vm((nz, batch, full), bf), vm((nz, max(1, ntp - 1), batch, width), bf),
        vm((nz, batch, width), bf), vm((nz, batch, width), bf),
        vm((nz, tok_count, width), bf), vm((nz, tok_count, width), bf),
        vm((2, batch, width), bf), vm((npl, top, tok_count), jnp.int32),
        vm((npl, tok_count, width), bf), vm((npl, tok_count, width), bf),
        vm((npl, tok_count, width), f32),
        dma((4,)), dma((3,)),
        dma((4, nz + 1)), dma((4, nz)),
        dma((2, nz)), dma((2, nz, max(1, npl - 1))), dma((2, nz)),
        dma((2, nz, max(1, ntp - 1))), dma((2, nz, max(1, ntp - 1))),
        dma((nz, max(1, ntp - 1))), dma((nz, max(1, ntp - 1))),
        dma((nz, 2)), dma((nz, 2)), dma((nz, 2)),
        dma((nz, 2)), dma((nz, 2)), dma((1,)), dma((2,)),
        dma((1,)), dma((1,)), dma((1,)), dma((1,)),
    ]
    inside = pl.BlockSpec(memory_space=pltpu.VMEM)
    outside = pl.BlockSpec(memory_space=pl.ANY)
    shapes = [tokens.shape, w_gate.shape, w_up.shape, w_down.shape]
    held = pl.pallas_call(
        functools.partial(kernel, nz, npl, ntp, cap),
        out_shape=tuple(vm(shape, bf) for shape in shapes),
        in_specs=[outside] * 7,
        out_specs=(inside,) * 4,
        scratch_shapes=scratch,
        compiler_params=pltpu.CompilerParams(
            collective_id=0, has_side_effects=True, vmem_limit_bytes=53 * 1024 * 1024
        ),
    )(tokens, cotangent, expert_ids.T, gate_values.T, w_gate, w_up, w_down)
    return pl.pallas_call(
        finish,
        out_shape=tuple(jax.ShapeDtypeStruct(shape, bf) for shape in shapes),
        in_specs=[inside] * 4,
        out_specs=(outside,) * 4,
        scratch_shapes=[dma((4,))],
        compiler_params=pltpu.CompilerParams(vmem_limit_bytes=1024 * 1024),
    )(*(pltpu.with_memory_space_constraint(value, pltpu.MemorySpace.VMEM) for value in held))


def solution(mesh):
    in_specs = (
        P("ep", "tp"), P("ep", "tp"), P("ep", None), P("ep", None),
        P("ep", "tp", None), P("ep", "tp", None), P("ep", "tp", None),
    )
    out_specs = (P("ep", "tp"), P("ep", "tp", None), P("ep", "tp", None), P("ep", "tp", None))
    body = functools.partial(local, mesh.shape["ep"], mesh.shape["tp"])
    return jax.shard_map(body, mesh=mesh, in_specs=in_specs, out_specs=out_specs, check_vma=False)
```
